32 devices in a mesh: dp: 16 (over z, y, x), mp: 2 (over core).
Axes of the slice: x: 2, y: 2, z: 4, core: 2. Of those that a mesh axis runs over, the one named last changes fastest.
Arguments:
- media: bfloat16 [256, 256, 1024], P('dp'), may hold values from -6 to 6
- slot_clip: int32 [256], P('dp'), may hold values from 0 to 15, as said below
- time_table: bfloat16 [144, 1024], replicated, may hold values from -6 to 6
- latents_init: float32 [64, 1024], replicated, may hold values from -6 to 6
- media_gain: float32 [2, 1024], replicated, may hold values from 0.5 to 1.5
- latent_gain: float32 [2, 1024], replicated, may hold values from 0.5 to 1.5
- final_gain: float32 [1024], replicated, may hold values from 0.5 to 1.5
- w_query: bfloat16 [2, 1024, 512], P(None, None, 'mp'), may hold values from -24 to 24
- w_key: bfloat16 [2, 1024, 512], P(None, None, 'mp'), may hold values from -0.1875 to 0.1875
- w_value: bfloat16 [2, 1024, 512], P(None, None, 'mp'), may hold values from -0.1875 to 0.1875
- w_out: bfloat16 [2, 512, 1024], P(None, 'mp'), may hold values from -0.5 to 0.5
Outputs:
- resampled: float32 [16, 64, 1024], P('dp')
The draws below stay inside these ranges and needn't reach their ends.
Inputs may be any that keep to these rules, and one draw needn't show every extreme that they name: `slot_clip`: slot b lies on dp index b // 16, and its clip differs from that index by at most 4; differences of +4 and -4 both occur in every draw.
All inputs are finite; a program needn't handle non-finite values.
Results may differ from the reference program's by a relative error of at most 0.0085.
The reference program's roundings to bfloat16 on the way count: a program that leaves them out, or rounds other values in their place, can miss the bound.
Values may be sent and summed in bfloat16 or wider, within the bound.
A program may use at most 128 MiB of HBM per device.

```python
import math
import jax
import jax.numpy as jnp
from jax import lax

D = 1024
HEADS = 8
HEAD_DIM = 64
LATENTS = 64
PATCHES = 256
LAYERS = 2
FRAMES_DEV = 16
REACH = 4
INNER = 512
CLIPS = 16
BLOCKS = 256
TIMES = 144
N_DP = 16


def draw_slot_clip(key, part):
    first, second, third, fourth = jax.random.split(jax.random.fold_in(key, 11), 4)
    pull = jax.random.randint(first, (CLIPS,), 1, 9)
    holder = jnp.arange(BLOCKS) // FRAMES_DEV
    shifts = jnp.arange(2 * REACH + 1) - REACH
    candidate = holder[:, None] + shifts[None, :]
    inside = (candidate >= 0) & (candidate < CLIPS)
    weights = jnp.where(inside, pull[jnp.clip(candidate, 0, CLIPS - 1)], 0)
    cumul = jnp.cumsum(weights, axis=1)
    ticket = jax.random.randint(second, (BLOCKS,), 0, 1048576) % cumul[:, -1]
    chosen = jnp.sum((cumul <= ticket[:, None]).astype(jnp.int32), axis=1)
    clip = jnp.take_along_axis(candidate, chosen[:, None], axis=1)[:, 0]
    upper = jax.random.randint(third, (), 0, CLIPS - REACH)
    lower = jax.random.randint(fourth, (), REACH, CLIPS)
    slots = jnp.arange(BLOCKS)
    clip = jnp.where(slots == upper * FRAMES_DEV, upper + REACH, clip)
    clip = jnp.where(slots == lower * FRAMES_DEV + FRAMES_DEV - 1, lower - REACH, clip)
    return clip.astype(jnp.int32)


def draw_w_query(key, part):
    base = jnp.clip(jax.random.normal(jax.random.fold_in(key, 5), (LAYERS, D, HEADS, HEAD_DIM), jnp.float32), -4.0, 4.0)
    scaled = base * 2.0 / math.sqrt(D)
    return scaled.reshape(LAYERS, D, HEADS * HEAD_DIM).astype(jnp.bfloat16)


def steps_of(key, shape, pieces, smallest, largest):
    loudness, own = 1.0, jax.random.fold_in(key, 6)
    for axis_at, parts in pieces:
        steps = jnp.exp(jax.random.uniform(jax.random.fold_in(own, axis_at), (parts,), jnp.float32, smallest / len(pieces), largest / len(pieces)))
        loudness = loudness * jnp.repeat(steps, shape[axis_at] // parts).reshape([-1 if axis == axis_at else 1 for axis in range(len(shape))])
    return loudness


def noise(own_key, shape, scale, reach, cuts=(), dtype=jnp.bfloat16):
    array = scale * jax.random.normal(own_key, shape, jnp.float32)
    if cuts:
        array = array * steps_of(own_key, shape, cuts, -0.22, 0.18)
    return jnp.clip(array, -reach, reach).astype(dtype)


def setup_inputs(seed: int = 0) -> dict:
    seeds = jax.random.split(jax.random.key(seed), 12)
    media = noise(seeds[0], (BLOCKS, PATCHES, D), 1.0, 6.0, ((0, 16),))
    slot_clip = draw_slot_clip(jax.random.fold_in(seeds[11], 71), 0)
    time_table = noise(seeds[2], (TIMES, D), 1.0, 6.0)
    latents_init = noise(seeds[3], (LATENTS, D), 1.0, 6.0, (), jnp.float32)
    media_gain = jnp.clip(1.0 + 0.1 * jax.random.normal(seeds[4], (LAYERS, D), jnp.float32), 0.5, 1.5)
    latent_gain = jnp.clip(1.0 + 0.1 * jax.random.normal(seeds[5], (LAYERS, D), jnp.float32), 0.5, 1.5)
    final_gain = jnp.clip(1.0 + 0.1 * jax.random.normal(seeds[6], (D,), jnp.float32), 0.5, 1.5)
    w_query = draw_w_query(jax.random.fold_in(seeds[11], 71), 0)
    w_key = noise(seeds[8], (LAYERS, D, INNER), D ** -0.5, 0.1875, ((2, 2),))
    w_value = noise(seeds[9], (LAYERS, D, INNER), D ** -0.5, 0.1875, ((2, 2),))
    w_out = noise(seeds[10], (LAYERS, INNER, D), (INNER // 4) ** -0.5, 0.5, ((1, 2),))
    return dict(media=media, slot_clip=slot_clip, time_table=time_table, latents_init=latents_init, media_gain=media_gain, latent_gain=latent_gain, final_gain=final_gain, w_query=w_query, w_key=w_key, w_value=w_value, w_out=w_out)


epsilon = 1e-05

def normalize(values):
    mean = lax.optimization_barrier(jnp.mean(values, axis=-1, keepdims=True))
    center = values - mean
    spread = lax.optimization_barrier(jnp.mean(center * center, axis=-1, keepdims=True))
    return center / jnp.sqrt(spread + epsilon)

def rounded(values):
    return lax.optimization_barrier(values.astype(jnp.bfloat16))

def block_stats(queries, keys, values):
    scores = jnp.einsum('qhd,khd->hqk', queries.astype(jnp.float32), keys.astype(jnp.float32))
    top = lax.optimization_barrier(jnp.max(scores, axis=-1))
    expo = jnp.exp(scores - top[..., None])
    total = lax.optimization_barrier(jnp.sum(expo, axis=-1))
    weights = rounded(expo).astype(jnp.float32)
    acc = jnp.einsum('hqk,khd->qhd', weights, values.astype(jnp.float32))
    return (top, total, acc)

def count_step(tally, clip):
    return (tally.at[clip].add(1), tally[clip])

def slot_stats(item):
    return block_stats(item[0], item[1], item[2])

def reference(media, slot_clip, time_table, latents_init, media_gain, latent_gain, final_gain, w_query, w_key, w_value, w_out):
    blocks, patches, width = media.shape
    clips = N_DP
    spent_tally, frame_index = lax.scan(count_step, jnp.zeros((clips,), jnp.int32), slot_clip)
    stamp = time_table[frame_index].astype(jnp.float32)
    unit = normalize(media.astype(jnp.float32) + stamp[:, None, :])
    state = jnp.broadcast_to(latents_init.astype(jnp.float32), (clips, LATENTS, width))
    for layer in range(LAYERS):
        lat_norm = rounded(normalize(state) * latent_gain[layer]).reshape(clips * LATENTS, width)
        query = rounded(jnp.dot(lat_norm, w_query[layer], preferred_element_type=jnp.float32) * HEAD_DIM ** (-0.5))
        query = query.reshape(clips, LATENTS, HEADS, HEAD_DIM)
        self_keys = rounded(jnp.dot(lat_norm, w_key[layer], preferred_element_type=jnp.float32)).reshape(clips, LATENTS, HEADS, HEAD_DIM)
        self_vals = rounded(jnp.dot(lat_norm, w_value[layer], preferred_element_type=jnp.float32)).reshape(clips, LATENTS, HEADS, HEAD_DIM)
        normed = rounded(unit * media_gain[layer]).reshape(blocks * patches, width)
        keys = rounded(jnp.dot(normed, w_key[layer], preferred_element_type=jnp.float32)).reshape(blocks, patches, HEADS, HEAD_DIM)
        vals = rounded(jnp.dot(normed, w_value[layer], preferred_element_type=jnp.float32)).reshape(blocks, patches, HEADS, HEAD_DIM)
        top, total, acc = lax.map(slot_stats, (query[slot_clip], keys, vals))
        own_top, own_total, own_acc = jax.vmap(block_stats)(query, self_keys, self_vals)
        best = own_top.at[slot_clip].max(top)
        weight = jnp.exp(top - best[slot_clip])
        own_weight = jnp.exp(own_top - best)
        whole = (own_weight * own_total).at[slot_clip].add(weight * total)
        combined = (own_acc * jnp.swapaxes(own_weight, 1, 2)[..., None]).at[slot_clip].add(acc * jnp.swapaxes(weight, 1, 2)[..., None])
        attn = rounded(combined / jnp.swapaxes(whole, 1, 2)[..., None]).reshape(clips * LATENTS, HEADS * HEAD_DIM)
        change = jnp.dot(attn, w_out[layer], preferred_element_type=jnp.float32)
        state = state + change.reshape(clips, LATENTS, width)
    return normalize(state) * final_gain
```

```python
import functools

import jax
import jax.numpy as jnp
from jax import lax
from jax.experimental import pallas as pl
from jax.experimental.pallas import tpu as pltpu
from jax.sharding import PartitionSpec as P

HEAD_DIM = 64
LAYERS = 2
REACH = 4
SPAN = 2 * REACH + 1
epsilon = 1e-05
floor_score = -1e30
F32 = jnp.float32
BF16 = jnp.bfloat16


def normalize(values):
    mean = jnp.mean(values, axis=-1, keepdims=True)
    center = values - mean
    spread = jnp.mean(center * center, axis=-1, keepdims=True)
    return center * lax.rsqrt(spread + epsilon)


def dot(a, b):
    return jnp.dot(a, b, preferred_element_type=F32)


def dot_nt(a, b):
    return lax.dot_general(a, b, (((1,), (1,)), ((), ())), preferred_element_type=F32)


def spread_heads(query, heads):
    column = lax.broadcasted_iota(jnp.int32, query.shape, 1) // HEAD_DIM
    zero = jnp.zeros_like(query)
    return jnp.concatenate([jnp.where(column == h, query, zero) for h in range(heads)], axis=0)


def compact(column, heads, rows):
    lane = lax.broadcasted_iota(jnp.int32, (rows, 128), 1) % heads
    tile = jnp.broadcast_to(column[:rows], (rows, 128))
    for h in range(1, heads):
        tile = jnp.where(lane == h, column[h * rows : (h + 1) * rows], tile)
    return tile


def expand(tile, heads):
    rows = tile.shape[0]
    column = lax.broadcasted_iota(jnp.int32, (rows, heads * HEAD_DIM), 1) // HEAD_DIM
    wide = jnp.broadcast_to(tile[:, 0:1], column.shape)
    for h in range(1, heads):
        wide = jnp.where(column == h, tile[:, h : h + 1], wide)
    return wide


def block_stats(wide_query, keys, values, heads, rows):
    scores = dot_nt(wide_query, keys)
    top = jnp.max(scores, axis=-1, keepdims=True)
    expo = jnp.exp(scores - top)
    total = jnp.sum(expo, axis=-1, keepdims=True)
    product = dot(expo.astype(BF16), values)
    column = lax.broadcasted_iota(jnp.int32, (rows, product.shape[1]), 1) // HEAD_DIM
    acc = product[:rows]
    for h in range(1, heads):
        acc = jnp.where(column == h, product[h * rows : (h + 1) * rows], acc)
    return compact(top, heads, rows), compact(total, heads, rows), acc


def kernel(
    clips,
    split,
    clip_ref,
    media_hbm,
    table_hbm,
    latents_ref,
    media_gain_ref,
    latent_gain_ref,
    final_gain_ref,
    wq_hbm,
    wk_hbm,
    wv_hbm,
    wo_hbm,
    out_ref,
    media,
    table,
    wq,
    wkv,
    wo,
    normed,
    keyvals,
    state,
    stamp,
    row_out,
    row_in,
    count,
    tops,
    totals,
    accs,
    slot_top,
    own_tile,
    own_acc,
    part_acc,
    part_stat,
    got_acc,
    got_stat,
    query_out,
    query_in,
    wide,
    change_out,
    change_in,
    media_sem,
    weight_sem,
    row_sems,
    part_sems,
    query_sems,
    change_sems,
):
    me = lax.axis_index("dp")
    core = lax.axis_index("mp")
    frames, patches, width = media_hbm.shape
    rows = latents_ref.shape[0]
    inner = wq_hbm.shape[2]
    heads = inner // HEAD_DIM

    def load(index, source, target):
        return pltpu.make_async_copy(source, target, weight_sem.at[index])

    left, right = pl.ds(0, inner), pl.ds(inner, inner)
    loads = [
        load(0, wq_hbm.at[0], wq.at[0]),
        load(1, wk_hbm.at[0], wkv.at[0, :, left]),
        load(2, wv_hbm.at[0], wkv.at[0, :, right]),
        load(3, table_hbm, table),
        load(4, wk_hbm.at[1], wkv.at[1, :, left]),
        load(5, wv_hbm.at[1], wkv.at[1, :, right]),
        load(6, wo_hbm, wo),
        load(7, wq_hbm.at[1], wq.at[1]),
    ]

    def media_copy(f):
        return pltpu.make_async_copy(media_hbm.at[f], media.at[f], media_sem.at[f])

    for copy in loads[:4]:
        copy.start()

    @pl.loop(0, frames)
    def _(f):
        media_copy(f).start()

    for copy in loads[4:]:
        copy.start()

    barrier = pltpu.get_barrier_semaphore()
    for k in range(1, 2 * REACH + 1):
        for step in (k, -k):
            target = me + step

            @pl.when((target >= 0) & (target < clips))
            def _():
                pl.semaphore_signal(barrier, inc=1, device_id={"dp": target})

    pl.semaphore_signal(barrier, inc=1, device_id={"mp": 1 - core})

    lane = lax.broadcasted_iota(jnp.int32, (frames, 128), 1)
    sub = lax.broadcasted_iota(jnp.int32, (frames, 128), 0)
    own_row = jnp.full((frames, 128), -1, jnp.int32)
    own_col = jnp.full((frames, 128), -1, jnp.int32)
    for f in range(frames):
        own_row = jnp.where(lane == f, clip_ref[f], own_row)
        own_col = jnp.where(sub == f, clip_ref[f], own_col)
    row_out[...] = own_row[:8]
    count[...] = ((own_row == own_col) & (lane < sub)).astype(jnp.int32)

    below = jnp.minimum(me, 2 * REACH)
    above = jnp.minimum(clips - 1 - me, 2 * REACH)
    pl.semaphore_wait(barrier, below + above + 1)

    def row_copy(k):
        return pltpu.make_async_remote_copy(
            src_ref=row_out,
            dst_ref=row_in.at[k - 1],
            send_sem=row_sems.at[0, k - 1],
            recv_sem=row_sems.at[1, k - 1],
            device_id={"dp": me + k},
        )

    for k in range(1, 2 * REACH + 1):

        @pl.when(me + k < clips)
        def _():
            row_copy(k).start()

    def self_block(layer, lat_norm, query):
        both = dot(lat_norm, wkv[layer]).astype(BF16)
        top, total, acc = block_stats(
            spread_heads(query, heads), both[:, :inner], both[:, inner:], heads, rows
        )
        own_tile[0] = top
        own_tile[1] = total
        own_acc[...] = acc

    def lat_query(layer, values):
        lat_norm = (normalize(values) * latent_gain_ref[layer : layer + 1]).astype(BF16)
        query = (dot(lat_norm, wq[layer]) * HEAD_DIM**-0.5).astype(BF16)
        return lat_norm, query

    loads[0].wait()
    state[...] = latents_ref[...]
    lat_norm, query = lat_query(0, latents_ref[...])
    loads[1].wait()
    loads[2].wait()
    wide[REACH] = spread_heads(query, heads)
    self_block(0, lat_norm, query)

    for k in range(1, 2 * REACH + 1):

        @pl.when(me - k >= 0)
        def _():
            row_copy(k).wait_recv()
            count[...] += (row_in[k - 1, 0:1] == own_col).astype(jnp.int32)

    frame_index = jnp.sum(count[...].astype(F32), axis=1, keepdims=True).astype(jnp.int32)
    loads[3].wait()
    times = lax.broadcasted_iota(jnp.int32, (frames, table.shape[0]), 1)
    picker = (times == frame_index).astype(F32).astype(BF16)
    stamp[...] = dot(picker, table[...])

    chunk = 32

    @pl.loop(0, frames)
    def _(f):
        media_copy(f).wait()
        added = stamp[pl.ds(f, 1)]
        gain_0, gain_1 = media_gain_ref[0:1], media_gain_ref[1:2]
        for start in range(0, patches, chunk):
            piece = pl.ds(start, chunk)
            unit = normalize(media[f, piece].astype(F32) + added)
            normed[piece] = (unit * gain_0).astype(BF16)
            media[f, piece] = (unit * gain_1).astype(BF16)
        both = dot(normed[...], wkv[0]).astype(BF16)
        top, total, acc = block_stats(wide[REACH], both[:, :inner], both[:, inner:], heads, rows)
        tops[f] = top
        totals[f] = total
        accs[f] = acc

    def slot_of(f):
        return jnp.clip(clip_ref[f] - me + REACH, 0, SPAN - 1)

    def part_copies(layer, slot):
        target = me + slot - REACH
        return [
            pltpu.make_async_remote_copy(
                src_ref=source.at[layer, slot],
                dst_ref=into.at[layer, slot],
                send_sem=part_sems.at[layer, 0, which, slot],
                recv_sem=part_sems.at[layer, 1, which, slot],
                device_id={"dp": target},
            )
            for which, (source, into) in enumerate(((part_acc, got_acc), (part_stat, got_stat)))
        ]

    lane_q = lax.broadcasted_iota(jnp.int32, (rows, 128), 1)
    order = [slot for k in range(REACH, 0, -1) for slot in (REACH - k, REACH + k)] + [REACH]

    def reduce_slots(layer):
        @pl.loop(0, SPAN)
        def _(slot):
            best = jnp.full((rows, 128), floor_score, F32)
            for f in range(frames):
                bias = jnp.where(clip_ref[f] - me + REACH == slot, 0.0, floor_score)
                best = jnp.maximum(best, tops[f] + bias)
            slot_top[slot] = best

        @pl.loop(0, frames)
        def _(f):
            weight = jnp.exp(tops[f] - slot_top[slot_of(f)])
            totals[f] = totals[f] * weight
            accs[f] = accs[f] * expand(weight, heads)

        for slot in order:
            share = [
                jnp.where(clip_ref[f] - me + REACH == slot, 1.0, 0.0).astype(F32)
                for f in range(frames)
            ]
            total = jnp.zeros((rows, 128), F32)
            acc = jnp.zeros((rows, inner), F32)
            for f in range(frames):
                total = total + totals[f] * share[f]
                acc = acc + accs[f] * share[f]
            part_acc[layer, slot] = acc.astype(BF16)
            part_stat[layer, slot] = jnp.where((lane_q // heads) % 2 == 0, slot_top[slot], total)
            if slot != REACH:
                target = me + slot - REACH

                @pl.when((target >= 0) & (target < clips))
                def _():
                    for copy in part_copies(layer, slot):
                        copy.start()

    def merge(layer):
        for slot in order:
            if slot != REACH:
                source = me - (slot - REACH)
                here = (source >= 0) & (source < clips)

                @pl.when(here)
                def _():
                    for copy in part_copies(layer, slot):
                        copy.wait_recv()

                @pl.when(jnp.logical_not(here))
                def _():
                    got_acc[layer, slot] = jnp.zeros((rows, inner), BF16)
                    got_stat[layer, slot] = jnp.where(
                        (lane_q // heads) % 2 == 0, floor_score, 0.0
                    ).astype(F32)

        def stat(slot):
            return part_stat[layer, slot] if slot == REACH else got_stat[layer, slot]

        best = own_tile[0]
        for slot in range(SPAN):
            best = jnp.maximum(best, stat(slot))
        own_weight = jnp.exp(own_tile[0] - best)
        whole = own_weight * own_tile[1]
        weights = []
        for slot in range(SPAN):
            tile = stat(slot)
            weight = jnp.exp(tile - best)
            weights.append(weight)
            whole = whole + weight * pltpu.roll(tile, heads, 1)
        inverse = 1.0 / whole
        combined = own_acc[...] * expand(own_weight * inverse, heads)
        for slot in range(SPAN):
            acc = part_acc[layer, slot] if slot == REACH else got_acc[layer, slot]
            combined = combined + acc.astype(F32) * expand(weights[slot] * inverse, heads)
        return combined.astype(BF16)

    def change_copy(layer):
        return pltpu.make_async_remote_copy(
            src_ref=change_out.at[layer],
            dst_ref=change_in.at[layer],
            send_sem=change_sems.at[0, layer],
            recv_sem=change_sems.at[1, layer],
            device_id={"mp": 1 - core},
        )

    def update(layer):
        change_out[layer] = dot(merge(layer), wo[layer]).astype(BF16)
        change_copy(layer).start()
        change_copy(layer).wait_recv()
        return state[...] + (change_out[layer].astype(F32) + change_in[layer].astype(F32))

    def project(f):
        keyvals[f] = dot(media[f], wkv[1]).astype(BF16)

    reduce_slots(0)
    loads[4].wait()
    loads[5].wait()
    pl.loop(0, split)(project)
    loads[6].wait()
    state[...] = update(0)

    loads[7].wait()
    lat_norm, query = lat_query(1, state[...])
    query_out[...] = query

    def query_copy(slot):
        return pltpu.make_async_remote_copy(
            src_ref=query_out,
            dst_ref=query_in.at[slot],
            send_sem=query_sems.at[0, slot],
            recv_sem=query_sems.at[1, slot],
            device_id={"dp": me - (slot - REACH)},
        )

    for slot in order[:-1]:
        target = me - (slot - REACH)

        @pl.when((target >= 0) & (target < clips))
        def _():
            query_copy(slot).start()

    wide[REACH] = spread_heads(query, heads)
    self_block(1, lat_norm, query)
    pl.loop(split, frames)(project)

    for slot in order[:-1]:
        source = me + slot - REACH

        @pl.when((source >= 0) & (source < clips))
        def _():
            query_copy(slot).wait_recv()
            wide[slot] = spread_heads(query_in[slot], heads)

    @pl.loop(0, frames)
    def _(f):
        top, total, acc = block_stats(
            wide[slot_of(f)],
            keyvals[f, :, :inner],
            keyvals[f, :, inner:],
            heads,
            rows,
        )
        tops[f] = top
        totals[f] = total
        accs[f] = acc

    reduce_slots(1)
    out_ref[0] = normalize(update(1)) * final_gain_ref[...]

    for k in range(1, 2 * REACH + 1):

        @pl.when(me + k < clips)
        def _():
            row_copy(k).wait_send()

    for slot in order[:-1]:
        target = me + slot - REACH

        @pl.when((target >= 0) & (target < clips))
        def _():
            for layer in range(LAYERS):
                for copy in part_copies(layer, slot):
                    copy.wait_send()

        other = me - (slot - REACH)

        @pl.when((other >= 0) & (other < clips))
        def _():
            query_copy(slot).wait_send()

    for layer in range(LAYERS):
        change_copy(layer).wait_send()


def local(
    media,
    slot_clip,
    time_table,
    latents_init,
    media_gain,
    latent_gain,
    final_gain,
    w_query,
    w_key,
    w_value,
    w_out,
):
    frames, patches, width = media.shape
    inner = w_query.shape[2]
    heads = inner // HEAD_DIM
    rows = latents_init.shape[0]
    clips = lax.axis_size("dp")
    split = 10 * frames // 16
    vmem = pl.BlockSpec(memory_space=pltpu.VMEM)
    hbm = pl.BlockSpec(memory_space=pl.ANY)
    dma = pltpu.SemaphoreType.DMA
    scratch = [
        pltpu.VMEM((frames, patches, width), BF16),
        pltpu.VMEM(time_table.shape, BF16),
        pltpu.VMEM(w_query.shape, BF16),
        pltpu.VMEM((LAYERS, width, 2 * inner), BF16),
        pltpu.VMEM(w_out.shape, BF16),
        pltpu.VMEM((patches, width), BF16),
        pltpu.VMEM((frames, patches, 2 * inner), BF16),
        pltpu.VMEM((rows, width), F32),
        pltpu.VMEM((frames, width), F32),
        pltpu.VMEM((8, 128), jnp.int32),
        pltpu.VMEM((2 * REACH, 8, 128), jnp.int32),
        pltpu.VMEM((frames, 128), jnp.int32),
        pltpu.VMEM((frames, rows, 128), F32),
        pltpu.VMEM((frames, rows, 128), F32),
        pltpu.VMEM((frames, rows, inner), F32),
        pltpu.VMEM((SPAN, rows, 128), F32),
        pltpu.VMEM((2, rows, 128), F32),
        pltpu.VMEM((rows, inner), F32),
        pltpu.VMEM((LAYERS, SPAN, rows, inner), BF16),
        pltpu.VMEM((LAYERS, SPAN, rows, 128), F32),
        pltpu.VMEM((LAYERS, SPAN, rows, inner), BF16),
        pltpu.VMEM((LAYERS, SPAN, rows, 128), F32),
        pltpu.VMEM((rows, inner), BF16),
        pltpu.VMEM((SPAN, rows, inner), BF16),
        pltpu.VMEM((SPAN, heads * rows, inner), BF16),
        pltpu.VMEM((LAYERS, rows, width), BF16),
        pltpu.VMEM((LAYERS, rows, width), BF16),
        dma((frames,)),
        dma((8,)),
        dma((2, 2 * REACH)),
        dma((LAYERS, 2, 2, SPAN)),
        dma((2, SPAN)),
        dma((2, LAYERS)),
    ]
    return pl.pallas_call(
        functools.partial(kernel, clips, split),
        out_shape=jax.ShapeDtypeStruct((1, rows, width), F32),
        in_specs=[
            pl.BlockSpec(memory_space=pltpu.SMEM),
            hbm,
            hbm,
            vmem,
            vmem,
            vmem,
            vmem,
            hbm,
            hbm,
            hbm,
            hbm,
        ],
        out_specs=vmem,
        scratch_shapes=scratch,
        compiler_params=pltpu.CompilerParams(
            collective_id=0, has_side_effects=True, vmem_limit_bytes=60 * 1024 * 1024
        ),
    )(
        slot_clip,
        media,
        time_table,
        latents_init,
        media_gain,
        latent_gain,
        final_gain[None],
        w_query,
        w_key,
        w_value,
        w_out,
    )


def solution(mesh):
    return jax.shard_map(
        local,
        mesh=mesh,
        in_specs=(
            P("dp", None, None),
            P("dp"),
            P(),
            P(),
            P(),
            P(),
            P(),
            P(None, None, "mp"),
            P(None, None, "mp"),
            P(None, None, "mp"),
            P(None, "mp", None),
        ),
        out_specs=P("dp", None, None),
        check_vma=False,
    )
```

```python
import functools

import jax
import jax.numpy as jnp
from jax import lax
from jax.experimental import pallas as pl
from jax.experimental.pallas import tpu as pltpu
from jax.sharding import PartitionSpec as P

HEAD_DIM = 64
LAYERS = 2
REACH = 4
SPAN = 2 * REACH + 1
epsilon = 1e-05
floor_score = -1e30
F32 = jnp.float32
BF16 = jnp.bfloat16


def normalize(values):
    mean = jnp.mean(values, axis=-1, keepdims=True)
    center = values - mean
    spread = jnp.mean(center * center, axis=-1, keepdims=True)
    return center * lax.rsqrt(spread + epsilon)


def dot(a, b):
    return jnp.dot(a, b, preferred_element_type=F32)


def dot_nt(a, b):
    return lax.dot_general(a, b, (((1,), (1,)), ((), ())), preferred_element_type=F32)


def spread_heads(query, heads):
    column = lax.broadcasted_iota(jnp.int32, query.shape, 1) // HEAD_DIM
    zero = jnp.zeros_like(query)
    return jnp.concatenate([jnp.where(column == h, query, zero) for h in range(heads)], axis=0)


def compact(column, heads, rows):
    lane = lax.broadcasted_iota(jnp.int32, (8, 128), 1)
    tile = jnp.zeros((8, 128), F32)
    for g in range(rows // 8):
        for h in range(heads):
            here = (lane // (2 * heads) == g) & (lane % heads == h)
            first = h * rows + 8 * g
            tile = jnp.where(here, column[first : first + 8], tile)
    return tile


def expand(tile, heads, rows):
    column = lax.broadcasted_iota(jnp.int32, (8, heads * HEAD_DIM), 1) // HEAD_DIM
    groups = []
    for g in range(rows // 8):
        first = 2 * heads * g
        wide = jnp.broadcast_to(tile[:, first : first + 1], column.shape)
        for h in range(1, heads):
            wide = jnp.where(column == h, tile[:, first + h : first + h + 1], wide)
        groups.append(wide)
    return jnp.concatenate(groups, axis=0)


def block_stats(wide_query, keys, values, heads, rows):
    scores = dot_nt(wide_query, keys)
    top = jnp.max(scores, axis=-1, keepdims=True)
    expo = jnp.exp(scores - top)
    total = jnp.sum(expo, axis=-1, keepdims=True)
    product = dot(expo.astype(BF16), values)
    column = lax.broadcasted_iota(jnp.int32, (rows, product.shape[1]), 1) // HEAD_DIM
    acc = product[:rows]
    for h in range(1, heads):
        acc = jnp.where(column == h, product[h * rows : (h + 1) * rows], acc)
    return compact(top, heads, rows), compact(total, heads, rows), acc


def kernel(
    clips,
    split,
    clip_ref,
    media_hbm,
    table_hbm,
    latents_ref,
    media_gain_ref,
    latent_gain_ref,
    final_gain_ref,
    wq_hbm,
    wk_hbm,
    wv_hbm,
    wo_hbm,
    out_ref,
    media,
    table,
    wq,
    wkv,
    wo,
    normed,
    keyvals,
    state,
    stamp,
    row_out,
    row_in,
    count,
    tops,
    totals,
    accs,
    slot_top,
    own_tile,
    own_acc,
    part_acc,
    part_stat,
    got_acc,
    got_stat,
    query_out,
    query_in,
    wide,
    change_out,
    change_in,
    media_sem,
    weight_sem,
    row_sems,
    part_sems,
    query_sems,
    change_sems,
):
    me = lax.axis_index("dp")
    core = lax.axis_index("mp")
    frames, patches, width = media_hbm.shape
    rows = latents_ref.shape[0]
    inner = wq_hbm.shape[2]
    heads = inner // HEAD_DIM

    def load(index, source, target):
        return pltpu.make_async_copy(source, target, weight_sem.at[index])

    left, right = pl.ds(0, inner), pl.ds(inner, inner)
    loads = [
        load(0, wq_hbm.at[0], wq.at[0]),
        load(1, wk_hbm.at[0], wkv.at[0, :, left]),
        load(2, wv_hbm.at[0], wkv.at[0, :, right]),
        load(3, table_hbm, table),
        load(4, wk_hbm.at[1], wkv.at[1, :, left]),
        load(5, wv_hbm.at[1], wkv.at[1, :, right]),
        load(6, wo_hbm, wo),
        load(7, wq_hbm.at[1], wq.at[1]),
    ]

    def media_copy(f):
        return pltpu.make_async_copy(media_hbm.at[f], media.at[f], media_sem.at[f])

    for copy in loads[:4]:
        copy.start()

    @pl.loop(0, frames)
    def _(f):
        media_copy(f).start()

    for copy in loads[4:]:
        copy.start()

    barrier = pltpu.get_barrier_semaphore()
    for k in range(1, 2 * REACH + 1):
        for step in (k, -k):
            target = me + step

            @pl.when((target >= 0) & (target < clips))
            def _():
                pl.semaphore_signal(barrier, inc=1, device_id={"dp": target})

    pl.semaphore_signal(barrier, inc=1, device_id={"mp": 1 - core})

    lane = lax.broadcasted_iota(jnp.int32, (frames, 128), 1)
    sub = lax.broadcasted_iota(jnp.int32, (frames, 128), 0)
    own_row = jnp.full((frames, 128), -1, jnp.int32)
    own_col = jnp.full((frames, 128), -1, jnp.int32)
    for f in range(frames):
        own_row = jnp.where(lane == f, clip_ref[f], own_row)
        own_col = jnp.where(sub == f, clip_ref[f], own_col)
    row_out[...] = own_row[:8]
    count[...] = ((own_row == own_col) & (lane < sub)).astype(jnp.int32)

    below = jnp.minimum(me, 2 * REACH)
    above = jnp.minimum(clips - 1 - me, 2 * REACH)
    pl.semaphore_wait(barrier, below + above + 1)

    def row_copy(k):
        return pltpu.make_async_remote_copy(
            src_ref=row_out,
            dst_ref=row_in.at[k - 1],
            send_sem=row_sems.at[0, k - 1],
            recv_sem=row_sems.at[1, k - 1],
            device_id={"dp": me + k},
        )

    for k in range(1, 2 * REACH + 1):

        @pl.when(me + k < clips)
        def _():
            row_copy(k).start()

    def self_block(layer, lat_norm, query):
        both = dot(lat_norm, wkv[layer]).astype(BF16)
        top, total, acc = block_stats(
            spread_heads(query, heads), both[:, :inner], both[:, inner:], heads, rows
        )
        own_tile[0] = top
        own_tile[1] = total
        own_acc[...] = acc

    def lat_query(layer, values):
        lat_norm = (normalize(values) * latent_gain_ref[layer : layer + 1]).astype(BF16)
        query = (dot(lat_norm, wq[layer]) * HEAD_DIM**-0.5).astype(BF16)
        return lat_norm, query

    loads[0].wait()
    state[...] = latents_ref[...]
    lat_norm, query = lat_query(0, latents_ref[...])
    loads[1].wait()
    loads[2].wait()
    wide[REACH] = spread_heads(query, heads)
    self_block(0, lat_norm, query)

    for k in range(1, 2 * REACH + 1):

        @pl.when(me - k >= 0)
        def _():
            row_copy(k).wait_recv()
            count[...] += (row_in[k - 1, 0:1] == own_col).astype(jnp.int32)

    frame_index = jnp.sum(count[...].astype(F32), axis=1, keepdims=True).astype(jnp.int32)
    loads[3].wait()
    times = lax.broadcasted_iota(jnp.int32, (frames, table.shape[0]), 1)
    picker = (times == frame_index).astype(F32).astype(BF16)
    stamp[...] = dot(picker, table[...])

    chunk = 16

    @pl.loop(0, frames)
    def _(f):
        media_copy(f).wait()
        added = stamp[pl.ds(f, 1)]
        gain_0, gain_1 = media_gain_ref[0:1], media_gain_ref[1:2]
        for start in range(0, patches, chunk):
            piece = pl.ds(start, chunk)
            unit = normalize(media[f, piece].astype(F32) + added)
            normed[piece] = (unit * gain_0).astype(BF16)
            media[f, piece] = (unit * gain_1).astype(BF16)
        both = dot(normed[...], wkv[0]).astype(BF16)
        top, total, acc = block_stats(wide[REACH], both[:, :inner], both[:, inner:], heads, rows)
        tops[f] = top
        totals[f] = total
        accs[f] = acc

    def slot_of(f):
        return jnp.clip(clip_ref[f] - me + REACH, 0, SPAN - 1)

    def part_copies(layer, slot):
        target = me + slot - REACH
        return [
            pltpu.make_async_remote_copy(
                src_ref=source.at[layer, slot],
                dst_ref=into.at[layer, slot],
                send_sem=part_sems.at[layer, 0, which, slot],
                recv_sem=part_sems.at[layer, 1, which, slot],
                device_id={"dp": target},
            )
            for which, (source, into) in enumerate(((part_acc, got_acc), (part_stat, got_stat)))
        ]

    lane_q = lax.broadcasted_iota(jnp.int32, (8, 128), 1)
    order = [slot for k in range(REACH, 0, -1) for slot in (REACH - k, REACH + k)] + [REACH]

    def reduce_slots(layer):
        @pl.loop(0, SPAN)
        def _(slot):
            best = jnp.full((8, 128), floor_score, F32)
            for f in range(frames):
                bias = jnp.where(clip_ref[f] - me + REACH == slot, 0.0, floor_score)
                best = jnp.maximum(best, tops[f] + bias)
            slot_top[slot] = best

        @pl.loop(0, frames)
        def _(f):
            weight = jnp.exp(tops[f] - slot_top[slot_of(f)])
            totals[f] = totals[f] * weight
            accs[f] = accs[f] * expand(weight, heads, rows)

        for slot in order:
            share = [
                jnp.where(clip_ref[f] - me + REACH == slot, 1.0, 0.0).astype(F32)
                for f in range(frames)
            ]
            total = jnp.zeros((8, 128), F32)
            acc = jnp.zeros((rows, inner), F32)
            for f in range(frames):
                total = total + totals[f] * share[f]
                acc = acc + accs[f] * share[f]
            part_acc[layer, slot] = acc.astype(BF16)
            part_stat[layer, slot] = jnp.where((lane_q // heads) % 2 == 0, slot_top[slot], total)
            if slot != REACH:
                target = me + slot - REACH

                @pl.when((target >= 0) & (target < clips))
                def _():
                    for copy in part_copies(layer, slot):
                        copy.start()

    def merge(layer):
        for slot in order:
            if slot != REACH:
                source = me - (slot - REACH)
                here = (source >= 0) & (source < clips)

                @pl.when(here)
                def _():
                    for copy in part_copies(layer, slot):
                        copy.wait_recv()

                @pl.when(jnp.logical_not(here))
                def _():
                    got_acc[layer, slot] = jnp.zeros((rows, inner), BF16)
                    got_stat[layer, slot] = jnp.where(
                        (lane_q // heads) % 2 == 0, floor_score, 0.0
                    ).astype(F32)

        def stat(slot):
            return part_stat[layer, slot] if slot == REACH else got_stat[layer, slot]

        best = own_tile[0]
        for slot in range(SPAN):
            best = jnp.maximum(best, stat(slot))
        own_weight = jnp.exp(own_tile[0] - best)
        whole = own_weight * own_tile[1]
        weights = []
        for slot in range(SPAN):
            tile = stat(slot)
            weight = jnp.exp(tile - best)
            weights.append(weight)
            whole = whole + weight * pltpu.roll(tile, 128 - heads, 1)
        inverse = 1.0 / whole
        combined = own_acc[...] * expand(own_weight * inverse, heads, rows)
        for slot in range(SPAN):
            acc = part_acc[layer, slot] if slot == REACH else got_acc[layer, slot]
            combined = combined + acc.astype(F32) * expand(weights[slot] * inverse, heads, rows)
        return combined.astype(BF16)

    def change_copy(layer):
        return pltpu.make_async_remote_copy(
            src_ref=change_out.at[layer],
            dst_ref=change_in.at[layer],
            send_sem=change_sems.at[0, layer],
            recv_sem=change_sems.at[1, layer],
            device_id={"mp": 1 - core},
        )

    def update(layer):
        change_out[layer] = dot(merge(layer), wo[layer]).astype(BF16)
        change_copy(layer).start()
        change_copy(layer).wait_recv()
        return state[...] + (change_out[layer].astype(F32) + change_in[layer].astype(F32))

    def project(f):
        keyvals[f] = dot(media[f], wkv[1]).astype(BF16)

    reduce_slots(0)
    loads[4].wait()
    loads[5].wait()
    pl.loop(0, split)(project)
    loads[6].wait()
    state[...] = update(0)

    loads[7].wait()
    lat_norm, query = lat_query(1, state[...])
    query_out[...] = query

    def query_copy(slot):
        return pltpu.make_async_remote_copy(
            src_ref=query_out,
            dst_ref=query_in.at[slot],
            send_sem=query_sems.at[0, slot],
            recv_sem=query_sems.at[1, slot],
            device_id={"dp": me - (slot - REACH)},
        )

    for slot in order[:-1]:
        target = me - (slot - REACH)

        @pl.when((target >= 0) & (target < clips))
        def _():
            query_copy(slot).start()

    wide[REACH] = spread_heads(query, heads)
    self_block(1, lat_norm, query)
    pl.loop(split, frames)(project)

    for slot in order[:-1]:
        source = me + slot - REACH

        @pl.when((source >= 0) & (source < clips))
        def _():
            query_copy(slot).wait_recv()
            wide[slot] = spread_heads(query_in[slot], heads)

    @pl.loop(0, frames)
    def _(f):
        top, total, acc = block_stats(
            wide[slot_of(f)],
            keyvals[f, :, :inner],
            keyvals[f, :, inner:],
            heads,
            rows,
        )
        tops[f] = top
        totals[f] = total
        accs[f] = acc

    reduce_slots(1)
    out_ref[0] = normalize(update(1)) * final_gain_ref[...]

    for k in range(1, 2 * REACH + 1):

        @pl.when(me + k < clips)
        def _():
            row_copy(k).wait_send()

    for slot in order[:-1]:
        target = me + slot - REACH

        @pl.when((target >= 0) & (target < clips))
        def _():
            for layer in range(LAYERS):
                for copy in part_copies(layer, slot):
                    copy.wait_send()

        other = me - (slot - REACH)

        @pl.when((other >= 0) & (other < clips))
        def _():
            query_copy(slot).wait_send()

    for layer in range(LAYERS):
        change_copy(layer).wait_send()


def local(
    media,
    slot_clip,
    time_table,
    latents_init,
    media_gain,
    latent_gain,
    final_gain,
    w_query,
    w_key,
    w_value,
    w_out,
):
    frames, patches, width = media.shape
    inner = w_query.shape[2]
    heads = inner // HEAD_DIM
    rows = latents_init.shape[0]
    clips = lax.axis_size("dp")
    split = 10 * frames // 16
    vmem = pl.BlockSpec(memory_space=pltpu.VMEM)
    hbm = pl.BlockSpec(memory_space=pl.ANY)
    dma = pltpu.SemaphoreType.DMA
    scratch = [
        pltpu.VMEM((frames, patches, width), BF16),
        pltpu.VMEM(time_table.shape, BF16),
        pltpu.VMEM(w_query.shape, BF16),
        pltpu.VMEM((LAYERS, width, 2 * inner), BF16),
        pltpu.VMEM(w_out.shape, BF16),
        pltpu.VMEM((patches, width), BF16),
        pltpu.VMEM((frames, patches, 2 * inner), BF16),
        pltpu.VMEM((rows, width), F32),
        pltpu.VMEM((frames, width), F32),
        pltpu.VMEM((8, 128), jnp.int32),
        pltpu.VMEM((2 * REACH, 8, 128), jnp.int32),
        pltpu.VMEM((frames, 128), jnp.int32),
        pltpu.VMEM((frames, 8, 128), F32),
        pltpu.VMEM((frames, 8, 128), F32),
        pltpu.VMEM((frames, rows, inner), F32),
        pltpu.VMEM((SPAN, 8, 128), F32),
        pltpu.VMEM((2, 8, 128), F32),
        pltpu.VMEM((rows, inner), F32),
        pltpu.VMEM((LAYERS, SPAN, rows, inner), BF16),
        pltpu.VMEM((LAYERS, SPAN, 8, 128), F32),
        pltpu.VMEM((LAYERS, SPAN, rows, inner), BF16),
        pltpu.VMEM((LAYERS, SPAN, 8, 128), F32),
        pltpu.VMEM((rows, inner), BF16),
        pltpu.VMEM((SPAN, rows, inner), BF16),
        pltpu.VMEM((SPAN, heads * rows, inner), BF16),
        pltpu.VMEM((LAYERS, rows, width), BF16),
        pltpu.VMEM((LAYERS, rows, width), BF16),
        dma((frames,)),
        dma((8,)),
        dma((2, 2 * REACH)),
        dma((LAYERS, 2, 2, SPAN)),
        dma((2, SPAN)),
        dma((2, LAYERS)),
    ]
    return pl.pallas_call(
        functools.partial(kernel, clips, split),
        out_shape=jax.ShapeDtypeStruct((1, rows, width), F32),
        in_specs=[
            pl.BlockSpec(memory_space=pltpu.SMEM),
            hbm,
            hbm,
            vmem,
            vmem,
            vmem,
            vmem,
            hbm,
            hbm,
            hbm,
            hbm,
        ],
        out_specs=vmem,
        scratch_shapes=scratch,
        compiler_params=pltpu.CompilerParams(
            collective_id=0, has_side_effects=True, vmem_limit_bytes=60 * 1024 * 1024
        ),
    )(
        slot_clip,
        media,
        time_table,
        latents_init,
        media_gain,
        latent_gain,
        final_gain[None],
        w_query,
        w_key,
        w_value,
        w_out,
    )


def solution(mesh):
    return jax.shard_map(
        local,
        mesh=mesh,
        in_specs=(
            P("dp", None, None),
            P("dp"),
            P(),
            P(),
            P(),
            P(),
            P(),
            P(None, None, "mp"),
            P(None, None, "mp"),
            P(None, None, "mp"),
            P(None, "mp", None),
        ),
        out_specs=P("dp", None, None),
        check_vma=False,
    )
```
